32 devices in a mesh: seq: 8 (over z, x), tp: 4 (over y, core).
Axes of the slice: x: 2, y: 2, z: 4, core: 2. Of those that a mesh axis runs over, the one named last changes fastest.
Arguments:
- queries: bfloat16 [1536, 6144], P('seq', 'tp'), may hold values from -400 to 400
- key_vectors: bfloat16 [1536, 1024], P('seq', 'tp'), may hold values from -8 to 8
- value_vectors: bfloat16 [1536, 1024], P('seq', 'tp'), may hold values from -6 to 6
- positions: int32 [1536], P('seq'), may hold values from 0 to 1535, as said below
- residual: bfloat16 [1536, 6144], P('seq', 'tp'), may hold values from -200 to 200
- norm_gain: float32 [1, 6144], P(None, 'tp'), may hold values from 0.5 to 1.5
- out_weight: bfloat16 [6144, 6144], P('tp'), may hold values from -0.3125 to 0.3125
Outputs:
- quantized: bfloat16 [1536, 6144], P('seq')
- token_scale: float32 [1536], P('seq')
- new_residual: bfloat16 [1536, 6144], P('seq', 'tp')
The draws below stay inside these ranges and needn't reach their ends.
Inputs may be any that keep to these rules, and one draw needn't show every extreme that they name: The positions are a permutation of 0 to 1535. Cut into 16 runs of 96 consecutive positions, the rows of one index of seq hold run r in their first 96 rows and run 2 * 8 - 1 - r in their last ones, both in increasing order, with r differing between the indices of seq.
All inputs are finite; a program needn't handle non-finite values. Where the reference program divides by a largest or mean magnitude, that divisor is 1e-20 or more.
Results may differ from the reference program's by a relative error of at most 0.012.
Values may be sent and summed in bfloat16 or wider, within the bound.
A program may use at most 64 MiB of HBM per device.

```python
import math
import jax
import jax.numpy as jnp
from jax import lax

D = 6144
Q_HEADS = 48
KV_HEADS = 8
HEAD = 128
TOK_DEV = 192
TOKENS = 1536
N_SEQ = 8
N_TP = 4


def shared_keys(key):
    inner_key = jax.random.fold_in(key, 21)
    shape = (TOKENS, KV_HEADS * HEAD)
    base_draw = jax.random.truncated_normal(inner_key, -5.0, 5.0, shape, jnp.float32)
    return base_draw


def draw_key_vectors(key, part):
    base_draw = shared_keys(key)
    return base_draw.astype(jnp.bfloat16)


def draw_queries(key, part):
    shape = (TOKENS, Q_HEADS * HEAD)
    noise_key = jax.random.fold_in(key, 23)
    base_draw = 2.0 * jax.random.truncated_normal(noise_key, -5.0, 5.0, shape, jnp.float32)
    return base_draw.astype(jnp.bfloat16)


def draw_positions(key, part):
    run_order = jax.random.permutation(jax.random.fold_in(key, 11), N_SEQ).astype(jnp.int32)
    half_rows = TOK_DEV // 2
    lane_index = jnp.arange(half_rows, dtype=jnp.int32)
    first_run = run_order[:, None] * half_rows + lane_index[None, :]
    second = (2 * N_SEQ - 1 - run_order)[:, None] * half_rows + lane_index[None, :]
    return jnp.concatenate([first_run, second], axis=1).reshape(TOKENS).astype(jnp.int32)


def draw_residual(key, part):
    noise_key = jax.random.fold_in(key, 31)
    column_key = jax.random.fold_in(key, 32)
    row_key = jax.random.fold_in(key, 33)
    column_index = jnp.arange(D, dtype=jnp.float32)
    column_scale = 3.0 ** (column_index / D) * jnp.exp(jax.random.uniform(column_key, (D,), jnp.float32, 0.0, 1.2))
    noise = jax.random.truncated_normal(noise_key, -5.0, 5.0, (TOKENS, D), jnp.float32)
    row_scale = jnp.exp(jax.random.uniform(row_key, (TOKENS, 1), jnp.float32, 0.0, math.log(10.0)))
    return (0.2 * noise * row_scale * column_scale[None, :]).astype(jnp.bfloat16)


def steps_of(stream_key, extent, shards, low, largest):
    gain, own = 1.0, jax.random.fold_in(stream_key, 6)
    for position, shards_of in shards:
        draws = jnp.exp(jax.random.uniform(jax.random.fold_in(own, position), (shards_of,), jnp.float32, low / len(shards), largest / len(shards)))
        gain = gain * jnp.repeat(draws, extent[position] // shards_of).reshape([-1 if axis == position else 1 for axis in range(len(extent))])
    return gain


def centred(stream_key, extent, scale, reach, shards=(), kind=jnp.bfloat16):
    loudness = steps_of(stream_key, extent, shards, -0.22, 0.18) if shards else 1.0
    values = jax.random.normal(stream_key, extent, jnp.float32) * scale * loudness
    return jnp.minimum(jnp.maximum(values, -reach), reach).astype(kind)


def setup_inputs(seed: int = 0) -> dict:
    splits = jax.random.split(jax.random.key(seed), 8)
    return {
        "queries": draw_queries(jax.random.fold_in(splits[7], 71), 0),
        "key_vectors": draw_key_vectors(jax.random.fold_in(splits[7], 71), 0),
        "value_vectors": centred(splits[2], (TOKENS, KV_HEADS * HEAD), 1.0, 6.0, ((0, 8), (1, 4))),
        "positions": draw_positions(jax.random.fold_in(splits[7], 71), 0),
        "residual": draw_residual(jax.random.fold_in(splits[7], 71), 0),
        "norm_gain": jnp.clip(1.0 + 0.1 * jax.random.normal(splits[5], (1, D), jnp.float32), 0.5, 1.5),
        "out_weight": centred(splits[6], (Q_HEADS * HEAD, D), (Q_HEADS * HEAD // 16) ** -0.5, 0.3125, ((0, 4),)),
    }


def reference(queries, key_vectors, value_vectors, positions, residual, norm_gain, out_weight):
    token_count = queries.shape[0]
    group_size = Q_HEADS // KV_HEADS
    score_scale = 1.0 / math.sqrt(HEAD)
    query_heads = queries.reshape(token_count, Q_HEADS, HEAD).transpose(1, 0, 2)
    key_heads = key_vectors.reshape(token_count, KV_HEADS, HEAD).transpose(1, 0, 2)
    value_heads = value_vectors.reshape(token_count, KV_HEADS, HEAD).transpose(1, 0, 2)
    block_rows = TOK_DEV
    block_count = token_count // block_rows
    query_blocks = query_heads.reshape(Q_HEADS, block_count, block_rows, HEAD)
    pos_blocks = positions.reshape(block_count, block_rows)

    def one_head(head_index):
        key_rows = key_heads[head_index // group_size]
        value_rows = value_heads[head_index // group_size]

        def one_block(block_pair):
            query_block, block_pos = block_pair
            scores = jnp.dot(query_block, key_rows.T, preferred_element_type=jnp.float32) * score_scale
            visible = positions[None, :] <= block_pos[:, None]
            scores = jnp.where(visible, scores, -1e+30)
            row_max = lax.optimization_barrier(jnp.max(scores, axis=1, keepdims=True))
            raw_weights = jnp.where(visible, jnp.exp(scores - row_max), 0.0)
            weight_sum = lax.optimization_barrier(jnp.sum(raw_weights, axis=1, keepdims=True))
            mixed = jnp.dot(raw_weights.astype(jnp.bfloat16), value_rows, preferred_element_type=jnp.float32)
            return (mixed / weight_sum).astype(jnp.bfloat16)
        return lax.map(one_block, (query_blocks[head_index], pos_blocks))
    attended = lax.map(one_head, jnp.arange(Q_HEADS, dtype=jnp.int32))
    attended = attended.reshape(Q_HEADS, token_count, HEAD).transpose(1, 0, 2).reshape(token_count, Q_HEADS * HEAD)
    group_width = Q_HEADS * HEAD // N_TP
    summed = residual.astype(jnp.float32)
    for group_index in range(N_TP):
        lower = group_index * group_width
        partial_value = jnp.dot(attended[:, lower:lower + group_width], out_weight[lower:lower + group_width], preferred_element_type=jnp.float32)
        partial_value = lax.optimization_barrier(partial_value.astype(jnp.bfloat16))
        summed = summed + partial_value.astype(jnp.float32)
    new_residual = summed.astype(jnp.bfloat16)
    mean_square = lax.optimization_barrier(jnp.mean(summed * summed, axis=1, keepdims=True))
    normed = summed * lax.rsqrt(mean_square + 1e-05) * norm_gain
    token_scale = lax.optimization_barrier(jnp.max(jnp.abs(normed), axis=1)) + 1e-06
    quantized = (normed / token_scale[:, None]).astype(jnp.bfloat16)
    return (quantized, token_scale, new_residual)
```

```python
import functools
import math

import jax
import jax.numpy as jnp
from jax import lax
from jax.experimental import pallas as pl
from jax.experimental.pallas import tpu as pltpu
from jax.sharding import PartitionSpec as P

HEAD = 128
LOG2E = 1.4426950408889634
MASKED = -1e30
MESH = pl.DeviceIdType.MESH
F32 = jnp.float32
BF16 = jnp.bfloat16


def kernel(
    dims,
    pos_ref, key_ref, value_ref, gain_ref, query_hbm, residual_hbm, weight_hbm,
    quant_hbm, scale_hbm, stream_hbm,
    kv, pos_all, gain_all, query_raw, residual_raw, query, residual, weight,
    attended, part, from_core, pair, gained, quant, stream, scale,
    load_sem, kv_send, kv_recv, forward_send, pos_send, pos_recv, gain_send, gain_recv,
    core_send, core_recv, y_send, y_recv, out_send, out_recv, out_local,
):
    n_seq, n_tp, group, kv_count, half, tile = dims
    n_y = n_tp // 2
    me = lax.axis_index("seq")
    tp = lax.axis_index("tp")
    core = lax.rem(tp, 2)
    y = tp // 2
    core_peer = tp + 1 - 2 * core
    partner = me + 1 - 2 * lax.rem(me, 2)
    model = weight.shape[1]
    tiles = model // tile
    slice_width = model // n_tp
    tiles_slice = slice_width // tile
    own = half // 2
    keys = n_seq * half

    loads = [
        pltpu.make_async_copy(query_hbm, query_raw, load_sem.at[0]),
        pltpu.make_async_copy(residual_hbm, residual_raw, load_sem.at[1]),
        pltpu.make_async_copy(weight_hbm, weight, load_sem.at[2]),
    ]
    for load in loads:
        load.start()

    barrier = pltpu.get_barrier_semaphore()
    for step in range(1, n_seq):
        pl.semaphore_signal(
            barrier, inc=1, device_id=(lax.rem(me + step, n_seq), tp), device_id_type=MESH
        )
    for step in range(1, n_tp):
        pl.semaphore_signal(
            barrier, inc=1, device_id=(me, lax.rem(tp + step, n_tp)), device_id_type=MESH
        )

    first = pos_ref[0:1, 0:1].astype(F32)
    second = pos_ref[0:1, half : half + 1].astype(F32)
    keep = jnp.where(first < second, 1.0, 0.0)

    def split(ref):
        top = ref[:half, :].astype(F32)
        bottom = ref[half:, :].astype(F32)
        low = top * keep + bottom * (1.0 - keep)
        high = bottom * keep + top * (1.0 - keep)
        return low.astype(BF16), high.astype(BF16)

    for index, ref in enumerate((key_ref, value_ref)):
        low, high = split(ref)
        kv[0, me, index] = low
        kv[1, me, index] = high
    pos_all[me] = pos_ref[...]
    gain_all[tp] = gain_ref[...]
    pl.semaphore_wait(barrier, n_seq + n_tp - 2)

    line = n_seq // 2
    order = []
    for step in range(1, line // 2 + 1):
        order.append(step)
        if line - step != step:
            order.append(line - step)
    sent = []

    def remote(src, dst, send, recv, device):
        copy = pltpu.make_async_remote_copy(
            src_ref=src, dst_ref=dst, send_sem=send, recv_sem=recv,
            device_id=device, device_id_type=MESH,
        )
        copy.start()
        sent.append(copy)
        return copy

    def landed(dst, recv):
        pltpu.make_async_remote_copy(
            src_ref=dst, dst_ref=dst, send_sem=recv, recv_sem=recv,
            device_id=(partner, tp), device_id_type=MESH,
        ).wait_recv()

    def send_line(phase):
        for step in order:
            target = lax.rem(me + 2 * step, n_seq)
            remote(
                kv.at[phase, me], kv.at[phase, me], kv_send.at[phase, step],
                kv_recv.at[phase, me], (target, tp),
            )

    def send_partner(phase):
        remote(
            kv.at[phase, me], kv.at[phase, me], kv_send.at[phase, 0],
            kv_recv.at[phase, me], (partner, tp),
        )

    def forward(phase, step):
        source = lax.rem(me + 2 * step, n_seq)
        landed(kv.at[phase, source], kv_recv.at[phase, source])
        remote(
            kv.at[phase, source], kv.at[phase, source], forward_send.at[phase, step],
            kv_recv.at[phase, source], (partner, tp),
        )

    def arrivals(phase):
        for step in range(line):
            source = lax.rem(partner + 2 * step, n_seq)
            landed(kv.at[phase, source], kv_recv.at[phase, source])

    send_partner(0)
    send_line(0)
    for step in range(1, n_seq):
        remote(
            pos_ref, pos_all.at[me], pos_send.at[step], pos_recv.at[me],
            (lax.rem(me + step, n_seq), tp),
        )
    for step in range(1, n_tp):
        remote(
            gain_ref, gain_all.at[tp], gain_send.at[step], gain_recv.at[tp],
            (me, lax.rem(tp + step, n_tp)),
        )
    loads[0].wait()
    loads[1].wait()
    query[0], query[1] = split(query_raw)
    residual[0], residual[1] = split(residual_raw)
    for step in order:
        forward(0, step)
    send_line(1)
    send_partner(1)
    for step in range(1, n_seq):
        source = lax.rem(me + step, n_seq)
        landed(pos_all.at[source], pos_recv.at[source])
    arrivals(0)

    lanes = lax.broadcasted_iota(jnp.int32, (1, keys), 1)
    rows = lax.broadcasted_iota(jnp.int32, (half, 1), 0).astype(F32)

    def bias(phase):
        pick = jnp.minimum if phase == 0 else jnp.maximum

        def base(index):
            value = pos_all[index]
            return pick(value[0:1, 0:1].astype(F32), value[0:1, half : half + 1].astype(F32))

        key_pos = jnp.zeros((1, keys), F32)
        for source in range(n_seq):
            inside = (lanes >= source * half) & (lanes < (source + 1) * half)
            key_pos = jnp.where(
                inside, base(source) + (lanes - source * half).astype(F32), key_pos
            )
        return jnp.where(key_pos <= base(me) + rows, 0.0, MASKED)

    stack = group if keys <= 1024 else 1

    def attend(phase):
        mask = bias(phase)
        for head in range(0, kv_count * group, stack):
            kv_head = head // group
            columns = slice(kv_head * HEAD, (kv_head + 1) * HEAD)
            block = jnp.concatenate(
                [
                    query[phase, :, (head + i) * HEAD : (head + i + 1) * HEAD]
                    for i in range(stack)
                ],
                axis=0,
            )
            scores = []
            for piece in range(phase + 1):
                key_rows = kv[piece, :, 0, :, columns].reshape(keys, HEAD)
                value = lax.dot_general(
                    block, key_rows, (((1,), (1,)), ((), ())), preferred_element_type=F32
                ).reshape(stack, half, keys)
                scores.append(value + mask[None] if piece == phase else value)
            peak = jnp.max(scores[0], axis=2, keepdims=True)
            for value in scores[1:]:
                peak = jnp.maximum(peak, jnp.max(value, axis=2, keepdims=True))
            mixed = jnp.zeros((stack * half, HEAD), F32)
            total = jnp.zeros((stack, half, 1), F32)
            for piece, value in enumerate(scores):
                weights = jnp.exp2((value - peak) * (LOG2E / math.sqrt(HEAD)))
                total += jnp.sum(weights, axis=2, keepdims=True)
                value_rows = kv[piece, :, 1, :, columns].reshape(keys, HEAD)
                mixed += jnp.dot(
                    weights.astype(BF16).reshape(stack * half, keys), value_rows,
                    preferred_element_type=F32,
                )
            mixed = (mixed.reshape(stack, half, HEAD) / total).astype(BF16)
            for i in range(stack):
                attended[phase, :, (head + i) * HEAD : (head + i + 1) * HEAD] = mixed[i]

    def reduce_tile(phase, index):
        landed(from_core.at[phase, index], core_recv.at[phase, index])
        both = part[phase, index, core].astype(F32) + from_core[phase, index].astype(F32)
        pair[phase, y, index] = both.astype(BF16)
        for step in range(1, n_y):
            target = lax.rem(y + step, n_y) * 2 + core
            remote(
                pair.at[phase, y, index], pair.at[phase, y, index],
                y_send.at[phase, index, step], y_recv.at[phase, y, index], (me, target),
            )

    def project(phase, between):
        for index in range(tiles):
            columns = slice(index * tile, (index + 1) * tile)
            product = jnp.dot(
                attended[phase], weight[:, columns], preferred_element_type=F32
            )
            inner = (index % tiles_slice) * tile
            mine = jnp.where(tp == index // tiles_slice, 1.0, 0.0)
            product += residual[phase, :, inner : inner + tile].astype(F32) * mine
            part[phase, index] = product.astype(BF16).reshape(2, own, tile)
            remote(
                part.at[phase, index, 1 - core], from_core.at[phase, index],
                core_send.at[phase, index], core_recv.at[phase, index], (me, core_peer),
            )
            if index >= 1:
                reduce_tile(phase, index - 1)
            if index < len(between):
                between[index]()
        reduce_tile(phase, tiles - 1)
        for task in between[tiles:]:
            task()

    locals_out = []

    def finish(phase):
        square = jnp.zeros((own, 1), F32)
        peak = jnp.zeros((own, 1), F32)
        for index in range(tiles):
            for step in range(1, n_y):
                source = lax.rem(y + step, n_y)
                landed(pair.at[phase, source, index], y_recv.at[phase, source, index])
            total = pair[phase, 0, index].astype(F32)
            for source in range(1, n_y):
                total += pair[phase, source, index].astype(F32)
            inner = (index % tiles_slice) * tile
            stream[phase, index // tiles_slice, :, inner : inner + tile] = total.astype(BF16)
            square += jnp.sum(total * total, axis=1, keepdims=True)
            scaled = total * gain_all[index // tiles_slice, :, inner : inner + tile]
            gained[index] = scaled
            peak = jnp.maximum(peak, jnp.max(jnp.abs(scaled), axis=1, keepdims=True))
        inverse = lax.rsqrt(square / model + 1e-5)
        token = inverse * peak + 1e-6
        factor = inverse / token
        scale[phase] = jnp.broadcast_to(token, (own, 128))
        for index in range(tiles):
            quant[phase, :, index * tile : (index + 1) * tile] = (gained[index] * factor).astype(
                BF16
            )
        sends = (
            (quant.at[phase], quant.at[phase], quant_hbm),
            (stream.at[phase, tp], stream.at[phase, core_peer], stream_hbm),
            (scale.at[phase], scale.at[phase], scale_hbm),
        )
        for index, (here, there, out) in enumerate(sends):
            remote(
                there, out.at[phase, core], out_send.at[phase, index],
                out_recv.at[phase, index], (me, core_peer),
            )
            copy = pltpu.make_async_copy(here, out.at[phase, core], out_local.at[phase, index])
            copy.start()
            locals_out.append(copy)

    attend(0)
    loads[2].wait()
    project(0, [functools.partial(forward, 1, step) for step in order])
    arrivals(1)
    attend(1)
    project(1, [])
    for step in range(1, n_tp):
        source = lax.rem(tp + step, n_tp)
        landed(gain_all.at[source], gain_recv.at[source])
    finish(0)
    finish(1)
    for phase in range(2):
        for index, out in enumerate((quant_hbm, stream_hbm, scale_hbm)):
            landed(out.at[phase, 1 - core], out_recv.at[phase, index])
    for copy in locals_out:
        copy.wait()
    for copy in sent:
        copy.wait_send()


def on_device(n_seq, n_tp, queries, key_vectors, value_vectors, positions, residual, norm_gain, out_weight):
    token_rows, query_width = queries.shape
    half = token_rows // 2
    own = half // 2
    kv_width = key_vectors.shape[1]
    kv_count = kv_width // HEAD
    group = query_width // kv_width
    model = out_weight.shape[1]
    slice_width = residual.shape[1]
    tile = math.gcd(slice_width, 768)
    tiles = model // tile
    n_y = n_tp // 2
    vmem = pl.BlockSpec(memory_space=pltpu.VMEM)
    anywhere = pl.BlockSpec(memory_space=pl.ANY)
    dma = pltpu.SemaphoreType.DMA
    line = n_seq // 2
    quant, scale, stream = pl.pallas_call(
        functools.partial(kernel, (n_seq, n_tp, group, kv_count, half, tile)),
        out_shape=(
            jax.ShapeDtypeStruct((2, 2, own, model), BF16),
            jax.ShapeDtypeStruct((2, 2, own, 128), F32),
            jax.ShapeDtypeStruct((2, 2, own, slice_width), BF16),
        ),
        in_specs=[vmem, vmem, vmem, vmem, anywhere, anywhere, anywhere],
        out_specs=(anywhere, anywhere, anywhere),
        scratch_shapes=[
            pltpu.VMEM((2, n_seq, 2, half, kv_width), BF16),
            pltpu.VMEM((n_seq, 1, token_rows), jnp.int32),
            pltpu.VMEM((n_tp, 1, slice_width), F32),
            pltpu.VMEM(queries.shape, BF16),
            pltpu.VMEM(residual.shape, BF16),
            pltpu.VMEM((2, half, query_width), BF16),
            pltpu.VMEM((2, half, slice_width), BF16),
            pltpu.VMEM(out_weight.shape, BF16),
            pltpu.VMEM((2, half, query_width), BF16),
            pltpu.VMEM((2, tiles, 2, own, tile), BF16),
            pltpu.VMEM((2, tiles, own, tile), BF16),
            pltpu.VMEM((2, n_y, tiles, own, tile), BF16),
            pltpu.VMEM((tiles, own, tile), F32),
            pltpu.VMEM((2, own, model), BF16),
            pltpu.VMEM((2, n_tp, own, slice_width), BF16),
            pltpu.VMEM((2, own, 128), F32),
            dma((3,)),
            dma((2, line)),
            dma((2, n_seq)),
            dma((2, line)),
            dma((n_seq,)),
            dma((n_seq,)),
            dma((n_tp,)),
            dma((n_tp,)),
            dma((2, tiles)),
            dma((2, tiles)),
            dma((2, tiles, n_y)),
            dma((2, n_y, tiles)),
            dma((2, 3)),
            dma((2, 3)),
            dma((2, 3)),
        ],
        compiler_params=pltpu.CompilerParams(
            collective_id=0, has_side_effects=True, vmem_limit_bytes=63 * 1024 * 1024
        ),
    )(positions[None, :], key_vectors, value_vectors, norm_gain, queries, residual, out_weight)
    ordered = positions[0] < positions[half]

    def restore(value):
        top = jnp.where(ordered, value[0], value[1])
        bottom = jnp.where(ordered, value[1], value[0])
        return jnp.stack((top, bottom)).reshape((token_rows,) + value.shape[3:])

    return (restore(quant), restore(scale[..., 0]), restore(stream))


def solution(mesh):
    return jax.shard_map(
        functools.partial(on_device, mesh.shape["seq"], mesh.shape["tp"]),
        mesh=mesh,
        in_specs=(
            P("seq", "tp"),
            P("seq", "tp"),
            P("seq", "tp"),
            P("seq"),
            P("seq", "tp"),
            P(None, "tp"),
            P("tp", None),
        ),
        out_specs=(P("seq", None), P("seq"), P("seq", "tp")),
        check_vma=False,
    )
```
